32 devices in a mesh: rows: 32 (over z, y, x, core).
Axes of the slice: x: 2, y: 2, z: 4, core: 2. Of those that a mesh axis runs over, the one named last changes fastest.
Arguments:
- source: float32 [64, 131072], P(None, 'rows'), may hold values from -6 to 6
- band_values: float32 [128, 131072], P(None, 'rows'), may hold values from -0.625 to 0.625
- offsets: int32 [128], replicated, may hold values from -128 to 128, as said below
Outputs:
- compressed: float32 [128, 131072], P(None, 'rows')
The draws below stay inside these ranges and needn't reach their ends.
Inputs may be any that keep to these rules, and one draw needn't show every extreme that they name: The 128 offsets are distinct and include both -128 and 128.
All inputs are finite; a program needn't handle non-finite values.
Results may differ from the reference program's by a relative error of at most 0.0003.
Values sent between devices are 32-bit elements; how exact they have to be, the bound alone decides.
A program may use at most 192 MiB of HBM per device.

```python
import jax
import jax.numpy as jnp
from jax import lax

ROWS_DEV = 4096
HB = 128
NB = 128
RB = 64
K1 = 128
K2 = 128
N = 131072
N_ROWS = 32


def draw_offsets(key, part):
    inner = jax.random.permutation(jax.random.fold_in(key, 11), 2 * HB - 1)[:NB - 2] - (HB - 1)
    ends = jnp.array([-HB, HB], jnp.int32)
    return jnp.concatenate([ends, inner.astype(jnp.int32)])


def steps_of(rng, dims, split, smallest, largest):
    gain, own = 1.0, jax.random.fold_in(rng, 6)
    for axis_at, parts in split:
        steps = jnp.exp(jax.random.uniform(jax.random.fold_in(own, axis_at), (parts,), jnp.float32, smallest / len(split), largest / len(split)))
        gain = gain * jnp.repeat(steps, dims[axis_at] // parts).reshape([-1 if axis == axis_at else 1 for axis in range(len(dims))])
    return gain


def bell_draw(own_key, dims, deviation, reach, split=(), kind=jnp.bfloat16):
    values = deviation * jax.random.normal(own_key, dims, jnp.float32)
    if split:
        values = values * steps_of(own_key, dims, split, -0.22, 0.18)
    return jnp.clip(values, -reach, reach).astype(kind)


def setup_inputs(seed: int = 0) -> dict:
    keys = jax.random.split(jax.random.key(seed), 4)
    source = bell_draw(keys[0], (RB, N), 1.0, 6.0, ((1, 32),), jnp.float32)
    band_values = bell_draw(keys[1], (NB, N), (0.5 / NB ** 0.5), 0.625, ((1, 32),), jnp.float32)
    offsets = draw_offsets(jax.random.fold_in(keys[3], 71), 0)
    return dict(source=source, band_values=band_values, offsets=offsets)


def band_blocks(band_values, offsets):
    diagonals = band_values.shape[0]
    blocks = band_values.shape[1] // HB
    values = band_values.reshape(diagonals, blocks, HB).transpose(1, 0, 2)
    within = jnp.arange(HB, dtype=jnp.int32)
    columns = within[None, :] + offsets[:, None].astype(jnp.int32) + HB
    row_index = jnp.broadcast_to(within[None, :], columns.shape)
    blocked = jnp.zeros((blocks, HB, 3 * HB), values.dtype)
    return blocked.at[:, row_index, columns].set(values)

def apply_band(extended, blocked):
    width = extended.shape[0]
    blocks = blocked.shape[0]
    pieces = extended.reshape(width, blocks + 2, HB)
    windows = jnp.concatenate([pieces[:, :-2], pieces[:, 1:-1], pieces[:, 2:]], axis=2)
    result = jnp.einsum('cbj,brj->cbr', windows, blocked, precision=lax.Precision.HIGHEST)
    return result.reshape(width, blocks * HB)

def apply_all(factor, band_values, offsets):
    width = factor.shape[0]
    padded = jnp.pad(factor, ((0, 0), (HB, HB)))

    def slab(index):
        start = (index * ROWS_DEV).astype(jnp.int32)
        anchor = jnp.zeros((), jnp.int32)
        piece = lax.dynamic_slice(padded, (anchor, start), (width, ROWS_DEV + 2 * HB))
        values = lax.dynamic_slice(band_values, (anchor, start), (band_values.shape[0], ROWS_DEV))
        return apply_band(piece, band_blocks(values, offsets))
    stacked = lax.map(slab, jnp.arange(N_ROWS, dtype=jnp.int32))
    return stacked.transpose(1, 0, 2).reshape(width, N_ROWS * ROWS_DEV)

def compress(grammian, retain):
    spanning = grammian[:, :retain]
    coeffs = None
    for repeat in range(2):
        if repeat > 0:
            spanning = jnp.dot(grammian, coeffs.T, precision=lax.Precision.HIGHEST)
        mapped = jnp.dot(grammian, spanning, precision=lax.Precision.HIGHEST)
        metric = jnp.dot(spanning.T, mapped, precision=lax.Precision.HIGHEST)
        metric = 0.5 * (metric + metric.T)
        factor = jnp.linalg.cholesky(metric)
        coeffs = jax.scipy.linalg.solve_triangular(factor, spanning.T, lower=True)
    return coeffs

def reference(source, band_values, offsets):
    total = source.shape[1]
    first = jnp.concatenate([source, apply_all(source, band_values, offsets)], axis=0)
    gram_one = jnp.dot(first, first.T, precision=lax.Precision.HIGHEST) / total
    coeffs_one = compress(gram_one, K1)
    factor = jnp.dot(coeffs_one, first, precision=lax.Precision.HIGHEST)
    once_more = apply_all(factor, band_values, offsets)
    squared = apply_all(once_more, band_values, offsets)
    second = jnp.concatenate([factor, squared], axis=0)
    gram_two = jnp.dot(second, second.T, precision=lax.Precision.HIGHEST) / total
    coeffs_two = compress(gram_two, K2)
    return jnp.dot(coeffs_two, second, precision=lax.Precision.HIGHEST)
```

```python
import functools

import jax
import jax.numpy as jnp
from jax import lax
from jax.experimental import pallas as pl
from jax.experimental.pallas import tpu as pltpu
from jax.sharding import PartitionSpec as P

HB = 128
K2 = 128
SUB = 8
MESH = pl.DeviceIdType.MESH
VMEM = pl.BlockSpec(memory_space=pltpu.VMEM)
ANY = pl.BlockSpec(memory_space=pl.ANY)
NT = (((1,), (1,)), ((), ()))


def exact(a, b, dims=(((1,), (0,)), ((), ()))):
    return lax.dot_general(
        a, b, dims, precision=lax.Precision.HIGHEST, preferred_element_type=jnp.float32
    )


def bf(a, b, dims=(((1,), (0,)), ((), ()))):
    return lax.dot_general(a, b, dims, preferred_element_type=jnp.float32)


def halves(value):
    high = value.astype(jnp.bfloat16)
    low = (value - high.astype(jnp.float32)).astype(jnp.bfloat16)
    return high, low


def halo_kernel(n, source, band, low_s, high_s, low_b, high_b, ls, hs, lb, hb, send, recv):
    me = lax.axis_index("rows")
    right, left = lax.rem(me + 1, n), lax.rem(me + n - 1, n)
    barrier = pltpu.get_barrier_semaphore()
    for neighbour in (left, right):
        pl.semaphore_signal(barrier, inc=1, device_id=(neighbour,), device_id_type=MESH)
    pl.semaphore_wait(barrier, 2)
    local = source.shape[1]
    deep_s, deep_b = ls.shape[1], lb.shape[1]
    moves = (
        (band.at[:, pl.ds(local - deep_b, deep_b)], lb, right),
        (band.at[:, pl.ds(0, deep_b)], hb, left),
        (source.at[:, pl.ds(local - deep_s, deep_s)], ls, right),
        (source.at[:, pl.ds(0, deep_s)], hs, left),
    )
    copies = []
    for index, (src, dst, target) in enumerate(moves):
        copies.append(
            pltpu.make_async_remote_copy(
                src_ref=src,
                dst_ref=dst,
                send_sem=send.at[index],
                recv_sem=recv.at[index],
                device_id=(target,),
                device_id_type=MESH,
            )
        )
    for copy in copies:
        copy.start()
    for copy in copies:
        copy.wait()
    low_b[...] = jnp.where(me > 0, lb[...], 0.0)
    high_b[...] = jnp.where(me < n - 1, hb[...], 0.0)
    low_s[...] = jnp.where(me > 0, ls[...], 0.0)
    high_s[...] = jnp.where(me < n - 1, hs[...], 0.0)


def halos(source, band):
    n = lax.axis_size("rows")
    shapes = [(source.shape[0], 3 * HB)] * 2 + [(band.shape[0], 2 * HB)] * 2
    return pl.pallas_call(
        functools.partial(halo_kernel, n),
        out_shape=[jax.ShapeDtypeStruct(shape, jnp.float32) for shape in shapes],
        in_specs=[ANY] * 2,
        out_specs=[VMEM] * 4,
        scratch_shapes=[pltpu.VMEM(shape, jnp.float32) for shape in shapes]
        + [pltpu.SemaphoreType.DMA((4,)), pltpu.SemaphoreType.DMA((4,))],
        compiler_params=pltpu.CompilerParams(collective_id=0, has_side_effects=True),
    )(source, band)


def total_kernel(n, owners, g, out, got, total, gathered, s1, r1, s2, r2):
    me = lax.axis_index("rows")
    stride = n // owners
    mine = me // stride
    barrier = pltpu.get_barrier_semaphore()

    def greet(k, _):
        pl.semaphore_signal(
            barrier, inc=1, device_id=(lax.rem(me + k, n),), device_id_type=MESH
        )
        return 0

    lax.fori_loop(1, n, greet, 0)
    pl.semaphore_wait(barrier, n - 1)

    def outward(o):
        return pltpu.make_async_remote_copy(
            src_ref=g.at[o],
            dst_ref=got.at[me],
            send_sem=s1.at[o],
            recv_sem=r1.at[me],
            device_id=(o * stride,),
            device_id_type=MESH,
        )

    def inward(other):
        return pltpu.make_async_remote_copy(
            src_ref=g.at[0],
            dst_ref=got.at[other],
            send_sem=s1.at[0],
            recv_sem=r1.at[other],
            device_id=(other,),
            device_id_type=MESH,
        )

    def back(other):
        return pltpu.make_async_remote_copy(
            src_ref=total,
            dst_ref=gathered.at[mine],
            send_sem=s2.at[other],
            recv_sem=r2.at[mine],
            device_id=(other,),
            device_id_type=MESH,
        )

    def spread(o):
        return pltpu.make_async_remote_copy(
            src_ref=total,
            dst_ref=gathered.at[o],
            send_sem=s2.at[0],
            recv_sem=r2.at[o],
            device_id=(o * stride,),
            device_id_type=MESH,
        )

    def send_out(k, _):
        o = lax.rem(mine + k, owners)

        @pl.when(o * stride != me)
        def _():
            outward(o).start()

        return 0

    lax.fori_loop(0, owners, send_out, 0)

    @pl.when(mine * stride == me)
    def _():
        got[me] = g[mine]

        def arrive(k, _):
            inward(lax.rem(me + k, n)).wait_recv()
            return 0

        lax.fori_loop(1, n, arrive, 0)
        summed = jnp.sum(got[...], axis=0)
        total[...] = summed
        gathered[mine] = summed

        def send_back(k, _):
            back(lax.rem(me + k, n)).start()
            return 0

        lax.fori_loop(1, n, send_back, 0)

    def collect(o, _):
        @pl.when(o * stride != me)
        def _():
            spread(o).wait_recv()
            outward(o).wait_send()

        return 0

    lax.fori_loop(0, owners, collect, 0)
    out[...] = gathered[...]

    @pl.when(mine * stride == me)
    def _():
        def sent(k, _):
            back(lax.rem(me + k, n)).wait_send()
            return 0

        lax.fori_loop(1, n, sent, 0)


def all_total(value, ident):
    n = lax.axis_size("rows")
    rows, columns = value.shape
    owners = rows // SUB
    shape = (owners, SUB, columns)
    dma = pltpu.SemaphoreType.DMA
    summed = pl.pallas_call(
        functools.partial(total_kernel, n, owners),
        out_shape=jax.ShapeDtypeStruct(shape, jnp.float32),
        in_specs=[VMEM],
        out_specs=VMEM,
        scratch_shapes=[
            pltpu.VMEM((n, SUB, columns), jnp.float32),
            pltpu.VMEM((SUB, columns), jnp.float32),
            pltpu.VMEM(shape, jnp.float32),
            dma((owners,)),
            dma((n,)),
            dma((n,)),
            dma((owners,)),
        ],
        compiler_params=pltpu.CompilerParams(collective_id=ident, has_side_effects=True),
    )(value.reshape(shape))
    return summed.reshape(rows, columns)


def banded(window_high, window_low, band_high, band_low):
    return (
        bf(window_high, band_high, NT)
        + bf(window_low, band_high, NT)
        + bf(window_high, band_low, NT)
    )


def columns_of(block, count=1):
    return pl.ds(pl.multiple_of(block * HB, HB), count * HB)


def first_kernel(
    source, band, offsets, low_s, high_s, low_b, high_b,
    first, upper, lower, gram, high, low, values
):
    width, local = source.shape
    blocks = upper.shape[0]
    for piece, at in ((low_s, 0), (source, 3 * HB), (high_s, 3 * HB + local)):
        part = piece[...]
        where = pl.ds(at, part.shape[1])
        top, bottom = halves(part)
        high[:, where] = top
        low[:, where] = bottom
    first[:width, pl.ds(0, 2 * HB)] = low_s[:, pl.ds(HB, 2 * HB)]
    first[:width, pl.ds(2 * HB, local)] = source[...]
    first[:width, pl.ds(2 * HB + local, 2 * HB)] = high_s[:, pl.ds(0, 2 * HB)]
    values[:, pl.ds(0, 2 * HB)] = low_b[...]
    values[:, pl.ds(2 * HB, local)] = band[...]
    values[:, pl.ds(2 * HB + local, 2 * HB)] = high_b[...]
    diagonals = band.shape[0]
    places = lax.broadcasted_iota(jnp.int32, (diagonals, 3 * HB), 1)
    chosen = jnp.where(places == offsets[...] + HB, 1.0, 0.0).astype(jnp.bfloat16)
    chosen = jnp.concatenate([chosen, chosen], axis=0)

    def step(block, _):
        top, bottom = halves(values[:, columns_of(block)].T)
        spread = bf(jnp.concatenate([top, bottom], axis=1), chosen)
        sheared = pltpu.roll(spread, 0, 1, stride=1, stride_axis=0)
        band_high, band_low = halves(sheared)
        upper[block] = band_high
        lower[block] = band_low
        window = columns_of(block, 3)
        first[width:, columns_of(block)] = banded(
            high[:, window], low[:, window], band_high, band_low
        )
        return 0

    lax.fori_loop(0, blocks, step, 0, unroll=2)
    inner = first[:, pl.ds(2 * HB, local)]
    gram[...] = exact(inner, inner, NT)


def make_first(source, band, offsets, edges):
    width, local = source.shape
    diagonals = band.shape[0]
    deep = local + 4 * HB
    blocks = deep // HB
    return pl.pallas_call(
        first_kernel,
        out_shape=[
            jax.ShapeDtypeStruct((2 * width, deep), jnp.float32),
            jax.ShapeDtypeStruct((blocks, HB, 3 * HB), jnp.bfloat16),
            jax.ShapeDtypeStruct((blocks, HB, 3 * HB), jnp.bfloat16),
            jax.ShapeDtypeStruct((2 * width, 2 * width), jnp.float32),
        ],
        in_specs=[VMEM] * 7,
        out_specs=[VMEM] * 4,
        scratch_shapes=[
            pltpu.VMEM((width, deep + 2 * HB), jnp.bfloat16),
            pltpu.VMEM((width, deep + 2 * HB), jnp.bfloat16),
            pltpu.VMEM((diagonals, deep), jnp.float32),
        ],
        compiler_params=pltpu.CompilerParams(vmem_limit_bytes=60 << 20),
    )(source, band, offsets.reshape(diagonals, 1), *edges)


def eliminate(metric, right):
    order = metric.shape[0]
    tiles = order // SUB
    s = [metric[SUB * t : SUB * t + SUB] for t in range(tiles)]
    y = [right[SUB * t : SUB * t + SUB] for t in range(tiles)]
    rows = lax.broadcasted_iota(jnp.int32, (SUB, 1), 0)
    for j in range(order):
        t0, r = divmod(j, SUB)
        scale = lax.rsqrt(s[t0][r : r + 1, j : j + 1])
        pivot_s = s[t0][r : r + 1] * scale
        pivot_y = y[t0][r : r + 1] * scale
        for t in range(t0, tiles):
            column = s[t][:, j : j + 1] * scale
            if t == t0:
                column = jnp.where(rows > r, column, 0.0)
                y[t] = jnp.where(rows == r, pivot_y, y[t])
            s[t] = s[t] - column * pivot_s
            y[t] = y[t] - column * pivot_y
    return jnp.concatenate(y, axis=0)


def compress(grammian, retain):
    spanning = grammian[:retain]
    coeffs = None
    for repeat in range(2):
        if repeat > 0:
            spanning = exact(coeffs, grammian)
        metric = exact(exact(spanning, grammian), spanning, NT)
        metric = 0.5 * (metric + metric.T)
        coeffs = eliminate(metric, spanning)
    return coeffs


def second_kernel(
    total, summed, first, upper, lower, factor, squared, corner, gram,
    high, low, once_high, once_low
):
    gram_one = summed[...] * (1.0 / total)
    keep = gram_one.shape[0]
    coeffs = compress(gram_one, keep)
    corner[...] = exact(exact(coeffs, gram_one), coeffs, NT)
    blocks = upper.shape[0]
    local = factor.shape[1]
    width = 4 * HB

    def expand(at, _):
        where = pl.ds(pl.multiple_of(at * width, width), width)
        top, bottom = halves(exact(coeffs, first[:, where]))
        high[:, where] = top
        low[:, where] = bottom
        return 0

    lax.fori_loop(0, first.shape[1] // width, expand, 0)

    def once(block, _):
        window = columns_of(block, 3)
        top, bottom = halves(
            banded(high[:, window], low[:, window], upper[block + 1], lower[block + 1])
        )
        once_high[:, columns_of(block)] = top
        once_low[:, columns_of(block)] = bottom
        return 0

    lax.fori_loop(0, blocks - 2, once, 0, unroll=2)

    def twice(block, _):
        window = columns_of(block, 3)
        squared[:, columns_of(block)] = banded(
            once_high[:, window], once_low[:, window], upper[block + 2], lower[block + 2]
        )
        return 0

    lax.fori_loop(0, blocks - 4, twice, 0, unroll=2)
    middle = pl.ds(2 * HB, local)
    factor[...] = high[:, middle].astype(jnp.float32) + low[:, middle].astype(jnp.float32)
    gram[:keep] = exact(factor[...], squared[...], NT)
    gram[keep:] = exact(squared[...], squared[...], NT)


def make_second(summed, first, upper, lower, total):
    keep, deep = first.shape
    local = deep - 4 * HB
    shape = jax.ShapeDtypeStruct
    return pl.pallas_call(
        functools.partial(second_kernel, total),
        out_shape=[
            shape((keep, local), jnp.float32),
            shape((keep, local), jnp.float32),
            shape((keep, keep), jnp.float32),
            shape((2 * keep, keep), jnp.float32),
        ],
        in_specs=[VMEM] * 4,
        out_specs=[VMEM] * 4,
        scratch_shapes=[
            pltpu.VMEM((keep, deep), jnp.bfloat16),
            pltpu.VMEM((keep, deep), jnp.bfloat16),
            pltpu.VMEM((keep, deep - 2 * HB), jnp.bfloat16),
            pltpu.VMEM((keep, deep - 2 * HB), jnp.bfloat16),
        ],
        compiler_params=pltpu.CompilerParams(vmem_limit_bytes=60 << 20),
    )(summed, first, upper, lower)


def last_kernel(total, summed, corner, factor, squared, out):
    keep = corner.shape[0]
    cross = summed[:keep] * (1.0 / total)
    own = summed[keep:] * (1.0 / total)
    top = jnp.concatenate([corner[...], cross], axis=1)
    bottom = jnp.concatenate([cross.T, own], axis=1)
    coeffs = compress(jnp.concatenate([top, bottom], axis=0), K2)
    width = 4 * HB

    def step(at, _):
        where = pl.ds(pl.multiple_of(at * width, width), width)
        stacked = jnp.concatenate([factor[:, where], squared[:, where]], axis=0)
        out[:, where] = exact(coeffs, stacked)
        return 0

    lax.fori_loop(0, out.shape[1] // width, step, 0)


def make_last(summed, corner, factor, squared, total):
    return pl.pallas_call(
        functools.partial(last_kernel, total),
        out_shape=jax.ShapeDtypeStruct((K2, factor.shape[1]), jnp.float32),
        in_specs=[VMEM] * 4,
        out_specs=VMEM,
        compiler_params=pltpu.CompilerParams(vmem_limit_bytes=60 << 20),
    )(summed, corner, factor, squared)


def body(source, band_values, offsets):
    total = float(source.shape[1] * lax.axis_size("rows"))
    edges = halos(source, band_values)
    first, upper, lower, gram = make_first(source, band_values, offsets, edges)
    summed = all_total(gram, 1)
    factor, squared, corner, gram = make_second(summed, first, upper, lower, total)
    summed = all_total(gram, 2)
    return make_last(summed, corner, factor, squared, total)


def solution(mesh):
    placed = (P(None, "rows"), P(None, "rows"), P())
    return jax.shard_map(
        body, mesh=mesh, in_specs=placed, out_specs=P(None, "rows"), check_vma=False
    )
```

```python
import functools

import jax
import jax.numpy as jnp
from jax import lax
from jax.experimental import pallas as pl
from jax.experimental.pallas import tpu as pltpu
from jax.sharding import PartitionSpec as P

HB = 128
K2 = 128
SUB = 8
LANE = 128
MESH = pl.DeviceIdType.MESH
VMEM = pl.BlockSpec(memory_space=pltpu.VMEM)
HBM = pl.BlockSpec(memory_space=pltpu.HBM)
NT = (((1,), (1,)), ((), ()))


def exact(a, b, dims=(((1,), (0,)), ((), ()))):
    return lax.dot_general(
        a, b, dims, precision=lax.Precision.HIGHEST, preferred_element_type=jnp.float32
    )


def bf(a, b, dims=(((1,), (0,)), ((), ()))):
    return lax.dot_general(a, b, dims, preferred_element_type=jnp.float32)


def halves(value):
    high = value.astype(jnp.bfloat16)
    low = (value - high.astype(jnp.float32)).astype(jnp.bfloat16)
    return high, low


def halo_kernel(n, source, band, low_s, high_s, low_b, high_b, ls, hs, lb, hb, send, recv):
    me = lax.axis_index("rows")
    right, left = lax.rem(me + 1, n), lax.rem(me + n - 1, n)
    barrier = pltpu.get_barrier_semaphore()
    for neighbour in (left, right):
        pl.semaphore_signal(barrier, inc=1, device_id=(neighbour,), device_id_type=MESH)
    pl.semaphore_wait(barrier, 2)
    local = source.shape[1]
    deep_s, deep_b = ls.shape[1], lb.shape[1]
    moves = (
        (band.at[:, pl.ds(local - deep_b, deep_b)], lb, right),
        (band.at[:, pl.ds(0, deep_b)], hb, left),
        (source.at[:, pl.ds(local - deep_s, deep_s)], ls, right),
        (source.at[:, pl.ds(0, deep_s)], hs, left),
    )
    copies = []
    for index, (src, dst, target) in enumerate(moves):
        copies.append(
            pltpu.make_async_remote_copy(
                src_ref=src,
                dst_ref=dst,
                send_sem=send.at[index],
                recv_sem=recv.at[index],
                device_id=(target,),
                device_id_type=MESH,
            )
        )
    for copy in copies:
        copy.start()
    for copy in copies:
        copy.wait()
    low_b[...] = jnp.where(me > 0, lb[...], 0.0)
    high_b[...] = jnp.where(me < n - 1, hb[...], 0.0)
    low_s[...] = jnp.where(me > 0, ls[...], 0.0)
    high_s[...] = jnp.where(me < n - 1, hs[...], 0.0)


def halos(source, band):
    n = lax.axis_size("rows")
    shapes = [(source.shape[0], 3 * HB)] * 2 + [(band.shape[0], 2 * HB)] * 2
    return pl.pallas_call(
        functools.partial(halo_kernel, n),
        out_shape=[jax.ShapeDtypeStruct(shape, jnp.float32) for shape in shapes],
        in_specs=[HBM] * 2,
        out_specs=[VMEM] * 4,
        scratch_shapes=[pltpu.VMEM(shape, jnp.float32) for shape in shapes]
        + [pltpu.SemaphoreType.DMA((4,)), pltpu.SemaphoreType.DMA((4,))],
        compiler_params=pltpu.CompilerParams(
            collective_id=0, has_side_effects=True, vmem_limit_bytes=8 << 20
        ),
    )(source, band)


def total_kernel(n, owners, g, out, got, total, gathered, s1, r1, s2, r2):
    me = lax.axis_index("rows")
    stride = n // owners
    mine = me // stride
    barrier = pltpu.get_barrier_semaphore()

    def greet(k, _):
        pl.semaphore_signal(
            barrier, inc=1, device_id=(lax.rem(me + k, n),), device_id_type=MESH
        )
        return 0

    lax.fori_loop(1, n, greet, 0)
    pl.semaphore_wait(barrier, n - 1)

    def outward(o):
        return pltpu.make_async_remote_copy(
            src_ref=g.at[o],
            dst_ref=got.at[me],
            send_sem=s1.at[o],
            recv_sem=r1.at[me],
            device_id=(o * stride,),
            device_id_type=MESH,
        )

    def inward(other):
        return pltpu.make_async_remote_copy(
            src_ref=g.at[0],
            dst_ref=got.at[other],
            send_sem=s1.at[0],
            recv_sem=r1.at[other],
            device_id=(other,),
            device_id_type=MESH,
        )

    def back(other):
        return pltpu.make_async_remote_copy(
            src_ref=total,
            dst_ref=gathered.at[mine],
            send_sem=s2.at[other],
            recv_sem=r2.at[mine],
            device_id=(other,),
            device_id_type=MESH,
        )

    def spread(o):
        return pltpu.make_async_remote_copy(
            src_ref=total,
            dst_ref=gathered.at[o],
            send_sem=s2.at[0],
            recv_sem=r2.at[o],
            device_id=(o * stride,),
            device_id_type=MESH,
        )

    def send_out(k, _):
        o = lax.rem(mine + k, owners)

        @pl.when(o * stride != me)
        def _():
            outward(o).start()

        return 0

    lax.fori_loop(0, owners, send_out, 0)

    @pl.when(mine * stride == me)
    def _():
        got[me] = g[mine]

        def arrive(k, _):
            inward(lax.rem(me + k, n)).wait_recv()
            return 0

        lax.fori_loop(1, n, arrive, 0)
        summed = jnp.sum(got[...], axis=0)
        total[...] = summed
        gathered[mine] = summed

        def send_back(k, _):
            back(lax.rem(me + k, n)).start()
            return 0

        lax.fori_loop(1, n, send_back, 0)

    def collect(o, _):
        @pl.when(o * stride != me)
        def _():
            spread(o).wait_recv()
            outward(o).wait_send()

        return 0

    lax.fori_loop(0, owners, collect, 0)
    out[...] = gathered[...]

    @pl.when(mine * stride == me)
    def _():
        def sent(k, _):
            back(lax.rem(me + k, n)).wait_send()
            return 0

        lax.fori_loop(1, n, sent, 0)


def all_total(value, ident):
    n = lax.axis_size("rows")
    rows, columns = value.shape
    owners = rows // SUB
    shape = (owners, SUB, columns)
    dma = pltpu.SemaphoreType.DMA
    summed = pl.pallas_call(
        functools.partial(total_kernel, n, owners),
        out_shape=jax.ShapeDtypeStruct(shape, jnp.float32),
        in_specs=[VMEM],
        out_specs=VMEM,
        scratch_shapes=[
            pltpu.VMEM((n, SUB, columns), jnp.float32),
            pltpu.VMEM((SUB, columns), jnp.float32),
            pltpu.VMEM(shape, jnp.float32),
            dma((owners,)),
            dma((n,)),
            dma((n,)),
            dma((owners,)),
        ],
        compiler_params=pltpu.CompilerParams(
            collective_id=ident, has_side_effects=True, vmem_limit_bytes=8 << 20
        ),
    )(value.reshape(shape))
    return summed.reshape(rows, columns)


def banded(window_high, window_low, band_high, band_low):
    return (
        bf(window_high, band_high, NT)
        + bf(window_low, band_high, NT)
        + bf(window_high, band_low, NT)
    )


def columns_of(block, count=1):
    return pl.ds(pl.multiple_of(block * HB, HB), count * HB)


def first_kernel(
    source, band, offsets, low_s, high_s, low_b, high_b,
    first, upper, lower, gram, high, low, values
):
    width, local = source.shape
    blocks = upper.shape[0]
    for piece, at in ((low_s, 0), (source, 3 * HB), (high_s, 3 * HB + local)):
        part = piece[...]
        where = pl.ds(at, part.shape[1])
        top, bottom = halves(part)
        high[:, where] = top
        low[:, where] = bottom
    first[:width, pl.ds(0, 2 * HB)] = low_s[:, pl.ds(HB, 2 * HB)]
    first[:width, pl.ds(2 * HB, local)] = source[...]
    first[:width, pl.ds(2 * HB + local, 2 * HB)] = high_s[:, pl.ds(0, 2 * HB)]
    values[:, pl.ds(0, 2 * HB)] = low_b[...]
    values[:, pl.ds(2 * HB, local)] = band[...]
    values[:, pl.ds(2 * HB + local, 2 * HB)] = high_b[...]
    diagonals = band.shape[0]
    places = lax.broadcasted_iota(jnp.int32, (diagonals, 3 * HB), 1)
    chosen = jnp.where(places == offsets[...] + HB, 1.0, 0.0).astype(jnp.bfloat16)
    chosen = jnp.concatenate([chosen, chosen], axis=0)

    def step(block, _):
        top, bottom = halves(values[:, columns_of(block)].T)
        spread = bf(jnp.concatenate([top, bottom], axis=1), chosen)
        sheared = pltpu.roll(spread, 0, 1, stride=1, stride_axis=0)
        band_high, band_low = halves(sheared)
        upper[block] = band_high
        lower[block] = band_low
        window = columns_of(block, 3)
        first[width:, columns_of(block)] = banded(
            high[:, window], low[:, window], band_high, band_low
        )
        return 0

    lax.fori_loop(0, blocks, step, 0, unroll=2)
    inner = first[:, pl.ds(2 * HB, local)]
    gram[...] = exact(inner, inner, NT)


def make_first(source, band, offsets, edges):
    width, local = source.shape
    diagonals = band.shape[0]
    deep = local + 4 * HB
    blocks = deep // HB
    return pl.pallas_call(
        first_kernel,
        out_shape=[
            jax.ShapeDtypeStruct((2 * width, deep), jnp.float32),
            jax.ShapeDtypeStruct((blocks, HB, 3 * HB), jnp.bfloat16),
            jax.ShapeDtypeStruct((blocks, HB, 3 * HB), jnp.bfloat16),
            jax.ShapeDtypeStruct((2 * width, 2 * width), jnp.float32),
        ],
        in_specs=[VMEM] * 7,
        out_specs=[VMEM] * 4,
        scratch_shapes=[
            pltpu.VMEM((width, deep + 2 * HB), jnp.bfloat16),
            pltpu.VMEM((width, deep + 2 * HB), jnp.bfloat16),
            pltpu.VMEM((diagonals, deep), jnp.float32),
        ],
        compiler_params=pltpu.CompilerParams(vmem_limit_bytes=28 << 20),
    )(source, band, offsets.reshape(diagonals, 1), *edges)


def splat(value):
    return jnp.broadcast_to(value, (SUB, LANE))


def eliminate(metric, right):
    tiles = metric.shape[0] // SUB
    part = [slice(SUB * t, SUB * t + SUB) for t in range(tiles)]
    state = [[metric[part[t]], right[part[t]]] for t in range(tiles)]
    rows = lax.broadcasted_iota(jnp.int32, (SUB, LANE), 0)
    solved = []
    steps = range(SUB)
    for t0 in range(tiles):
        at = SUB * t0
        core = {
            (i, k): splat(state[t0][0][i : i + 1, at + k : at + k + 1])
            for i in steps
            for k in range(i, SUB)
        }
        pivots = [[splat(half[i : i + 1]) for half in state[t0]] for i in steps]
        inverse = []
        for i in steps:
            inverse.append(1.0 / core[i, i])
            for k in range(i + 1, SUB):
                ratio = core[i, k] * inverse[i]
                for m in range(k, SUB):
                    core[k, m] = core[k, m] - ratio * core[i, m]
                pivots[k] = [p - ratio * q for p, q in zip(pivots[k], pivots[i])]
        result = jnp.zeros((SUB, LANE), jnp.float32)
        for i in steps:
            result = jnp.where(rows == i, pivots[i][1] * lax.rsqrt(core[i, i]), result)
        solved.append(result)
        for t in range(t0 + 1, tiles):
            scaled = []
            for k in steps:
                column = splat(state[t][0][:, at + k : at + k + 1])
                for i in range(k):
                    column = column - scaled[i] * core[i, k]
                scaled.append(column * inverse[k])
            for half in range(2):
                value = state[t][half]
                for k in steps:
                    value = value - scaled[k] * pivots[k][half]
                state[t][half] = value
    return jnp.concatenate(solved, axis=0)


def compress(grammian, retain):
    spanning = grammian[:retain]
    wide = spanning.shape[1] > retain
    across = lax.broadcasted_iota(jnp.int32, (retain, retain), 1)
    down = lax.broadcasted_iota(jnp.int32, (retain, retain), 0)
    unit = jnp.where(across == down, 1.0, 0.0)
    coeffs = None
    for repeat in range(2):
        if repeat > 0:
            spanning = exact(coeffs, grammian)
        metric = exact(exact(spanning, grammian), spanning, NT)
        metric = 0.5 * (metric + metric.T)
        if wide:
            coeffs = exact(eliminate(metric, unit), spanning)
        else:
            coeffs = eliminate(metric, spanning)
    return coeffs


def second_kernel(
    total, summed, first, upper, lower, factor, squared, corner, gram,
    high, low, once_high, once_low
):
    gram_one = summed[...] * (1.0 / total)
    keep = gram_one.shape[0]
    coeffs = compress(gram_one, keep)
    corner[...] = exact(exact(coeffs, gram_one), coeffs, NT)
    blocks = upper.shape[0]
    local = factor.shape[1]
    width = 4 * HB

    def expand(at, _):
        where = pl.ds(pl.multiple_of(at * width, width), width)
        top, bottom = halves(exact(coeffs, first[:, where]))
        high[:, where] = top
        low[:, where] = bottom
        return 0

    lax.fori_loop(0, first.shape[1] // width, expand, 0)

    def once(block, _):
        window = columns_of(block, 3)
        top, bottom = halves(
            banded(high[:, window], low[:, window], upper[block + 1], lower[block + 1])
        )
        once_high[:, columns_of(block)] = top
        once_low[:, columns_of(block)] = bottom
        return 0

    lax.fori_loop(0, blocks - 2, once, 0, unroll=2)

    def twice(block, _):
        window = columns_of(block, 3)
        squared[:, columns_of(block)] = banded(
            once_high[:, window], once_low[:, window], upper[block + 2], lower[block + 2]
        )
        return 0

    lax.fori_loop(0, blocks - 4, twice, 0, unroll=2)
    middle = pl.ds(2 * HB, local)
    factor[...] = high[:, middle].astype(jnp.float32) + low[:, middle].astype(jnp.float32)
    gram[:keep] = exact(factor[...], squared[...], NT)
    gram[keep:] = exact(squared[...], squared[...], NT)


def make_second(summed, first, upper, lower, total):
    keep, deep = first.shape
    local = deep - 4 * HB
    shape = jax.ShapeDtypeStruct
    return pl.pallas_call(
        functools.partial(second_kernel, total),
        out_shape=[
            shape((keep, local), jnp.float32),
            shape((keep, local), jnp.float32),
            shape((keep, keep), jnp.float32),
            shape((2 * keep, keep), jnp.float32),
        ],
        in_specs=[VMEM] * 4,
        out_specs=[VMEM] * 4,
        scratch_shapes=[
            pltpu.VMEM((keep, deep), jnp.bfloat16),
            pltpu.VMEM((keep, deep), jnp.bfloat16),
            pltpu.VMEM((keep, deep - 2 * HB), jnp.bfloat16),
            pltpu.VMEM((keep, deep - 2 * HB), jnp.bfloat16),
        ],
        compiler_params=pltpu.CompilerParams(vmem_limit_bytes=28 << 20),
    )(summed, first, upper, lower)


def last_kernel(total, summed, corner, factor, squared, out):
    keep = corner.shape[0]
    cross = summed[:keep] * (1.0 / total)
    own = summed[keep:] * (1.0 / total)
    top = jnp.concatenate([corner[...], cross], axis=1)
    bottom = jnp.concatenate([cross.T, own], axis=1)
    coeffs = compress(jnp.concatenate([top, bottom], axis=0), K2)
    width = 4 * HB

    def step(at, _):
        where = pl.ds(pl.multiple_of(at * width, width), width)
        stacked = jnp.concatenate([factor[:, where], squared[:, where]], axis=0)
        out[:, where] = exact(coeffs, stacked)
        return 0

    lax.fori_loop(0, out.shape[1] // width, step, 0)


def make_last(summed, corner, factor, squared, total):
    return pl.pallas_call(
        functools.partial(last_kernel, total),
        out_shape=jax.ShapeDtypeStruct((K2, factor.shape[1]), jnp.float32),
        in_specs=[VMEM] * 4,
        out_specs=VMEM,
        compiler_params=pltpu.CompilerParams(vmem_limit_bytes=28 << 20),
    )(summed, corner, factor, squared)


def body(source, band_values, offsets):
    total = float(source.shape[1] * lax.axis_size("rows"))
    edges = halos(source, band_values)
    first, upper, lower, gram = make_first(source, band_values, offsets, edges)
    summed = all_total(gram, 1)
    factor, squared, corner, gram = make_second(summed, first, upper, lower, total)
    summed = all_total(gram, 2)
    return make_last(summed, corner, factor, squared, total)


def solution(mesh):
    placed = (P(None, "rows"), P(None, "rows"), P())
    return jax.shard_map(
        body, mesh=mesh, in_specs=placed, out_specs=P(None, "rows"), check_vma=False
    )
```

```python
import functools

import jax
import jax.numpy as jnp
from jax import lax
from jax.experimental import pallas as pl
from jax.experimental.pallas import tpu as pltpu
from jax.sharding import PartitionSpec as P

HB = 128
K2 = 128
SUB = 8
LANE = 128
MESH = pl.DeviceIdType.MESH
VMEM = pl.BlockSpec(memory_space=pltpu.VMEM)
HBM = pl.BlockSpec(memory_space=pltpu.HBM)
NT = (((1,), (1,)), ((), ()))


def exact(a, b, dims=(((1,), (0,)), ((), ()))):
    return lax.dot_general(
        a, b, dims, precision=lax.Precision.HIGHEST, preferred_element_type=jnp.float32
    )


def bf(a, b, dims=(((1,), (0,)), ((), ()))):
    return lax.dot_general(a, b, dims, preferred_element_type=jnp.float32)


def halves(value):
    high = value.astype(jnp.bfloat16)
    low = (value - high.astype(jnp.float32)).astype(jnp.bfloat16)
    return high, low


def halo_kernel(n, source, band, low_s, high_s, low_b, high_b, ls, hs, lb, hb, send, recv):
    me = lax.axis_index("rows")
    right, left = lax.rem(me + 1, n), lax.rem(me + n - 1, n)
    barrier = pltpu.get_barrier_semaphore()
    for neighbour in (left, right):
        pl.semaphore_signal(barrier, inc=1, device_id=(neighbour,), device_id_type=MESH)
    pl.semaphore_wait(barrier, 2)
    local = source.shape[1]
    deep_s, deep_b = ls.shape[1], lb.shape[1]
    moves = (
        (band.at[:, pl.ds(local - deep_b, deep_b)], lb, right),
        (band.at[:, pl.ds(0, deep_b)], hb, left),
        (source.at[:, pl.ds(local - deep_s, deep_s)], ls, right),
        (source.at[:, pl.ds(0, deep_s)], hs, left),
    )
    copies = []
    for index, (src, dst, target) in enumerate(moves):
        copies.append(
            pltpu.make_async_remote_copy(
                src_ref=src,
                dst_ref=dst,
                send_sem=send.at[index],
                recv_sem=recv.at[index],
                device_id=(target,),
                device_id_type=MESH,
            )
        )
    for copy in copies:
        copy.start()
    for copy in copies:
        copy.wait()
    low_b[...] = jnp.where(me > 0, lb[...], 0.0)
    high_b[...] = jnp.where(me < n - 1, hb[...], 0.0)
    low_s[...] = jnp.where(me > 0, ls[...], 0.0)
    high_s[...] = jnp.where(me < n - 1, hs[...], 0.0)


def halos(source, band):
    n = lax.axis_size("rows")
    shapes = [(source.shape[0], 3 * HB)] * 2 + [(band.shape[0], 2 * HB)] * 2
    return pl.pallas_call(
        functools.partial(halo_kernel, n),
        out_shape=[jax.ShapeDtypeStruct(shape, jnp.float32) for shape in shapes],
        in_specs=[HBM] * 2,
        out_specs=[VMEM] * 4,
        scratch_shapes=[pltpu.VMEM(shape, jnp.float32) for shape in shapes]
        + [pltpu.SemaphoreType.DMA((4,)), pltpu.SemaphoreType.DMA((4,))],
        compiler_params=pltpu.CompilerParams(
            collective_id=0, has_side_effects=True, vmem_limit_bytes=8 << 20
        ),
    )(source, band)


def total_kernel(n, owners, g, out, got, total, gathered, s1, r1, s2, r2):
    me = lax.axis_index("rows")
    stride = n // owners
    mine = me // stride
    barrier = pltpu.get_barrier_semaphore()

    def greet(k, _):
        pl.semaphore_signal(
            barrier, inc=1, device_id=(lax.rem(me + k, n),), device_id_type=MESH
        )
        return 0

    lax.fori_loop(1, n, greet, 0)
    pl.semaphore_wait(barrier, n - 1)

    def outward(o):
        return pltpu.make_async_remote_copy(
            src_ref=g.at[o],
            dst_ref=got.at[me],
            send_sem=s1.at[o],
            recv_sem=r1.at[me],
            device_id=(o * stride,),
            device_id_type=MESH,
        )

    def inward(other):
        return pltpu.make_async_remote_copy(
            src_ref=g.at[0],
            dst_ref=got.at[other],
            send_sem=s1.at[0],
            recv_sem=r1.at[other],
            device_id=(other,),
            device_id_type=MESH,
        )

    def back(other):
        return pltpu.make_async_remote_copy(
            src_ref=total,
            dst_ref=gathered.at[mine],
            send_sem=s2.at[other],
            recv_sem=r2.at[mine],
            device_id=(other,),
            device_id_type=MESH,
        )

    def spread(o):
        return pltpu.make_async_remote_copy(
            src_ref=total,
            dst_ref=gathered.at[o],
            send_sem=s2.at[0],
            recv_sem=r2.at[o],
            device_id=(o * stride,),
            device_id_type=MESH,
        )

    def send_out(k, _):
        o = lax.rem(mine + k, owners)

        @pl.when(o * stride != me)
        def _():
            outward(o).start()

        return 0

    lax.fori_loop(0, owners, send_out, 0)

    @pl.when(mine * stride == me)
    def _():
        got[me] = g[mine]

        def arrive(k, _):
            inward(lax.rem(me + k, n)).wait_recv()
            return 0

        lax.fori_loop(1, n, arrive, 0)
        summed = jnp.sum(got[...], axis=0)
        total[...] = summed
        gathered[mine] = summed

        def send_back(k, _):
            back(lax.rem(me + k, n)).start()
            return 0

        lax.fori_loop(1, n, send_back, 0)

    def collect(o, _):
        @pl.when(o * stride != me)
        def _():
            spread(o).wait_recv()
            outward(o).wait_send()

        return 0

    lax.fori_loop(0, owners, collect, 0)
    out[...] = gathered[...]

    @pl.when(mine * stride == me)
    def _():
        def sent(k, _):
            back(lax.rem(me + k, n)).wait_send()
            return 0

        lax.fori_loop(1, n, sent, 0)


def all_total(value, ident):
    n = lax.axis_size("rows")
    rows, columns = value.shape
    owners = rows // SUB
    shape = (owners, SUB, columns)
    dma = pltpu.SemaphoreType.DMA
    summed = pl.pallas_call(
        functools.partial(total_kernel, n, owners),
        out_shape=jax.ShapeDtypeStruct(shape, jnp.float32),
        in_specs=[VMEM],
        out_specs=VMEM,
        scratch_shapes=[
            pltpu.VMEM((n, SUB, columns), jnp.float32),
            pltpu.VMEM((SUB, columns), jnp.float32),
            pltpu.VMEM(shape, jnp.float32),
            dma((owners,)),
            dma((n,)),
            dma((n,)),
            dma((owners,)),
        ],
        compiler_params=pltpu.CompilerParams(
            collective_id=ident, has_side_effects=True, vmem_limit_bytes=8 << 20
        ),
    )(value.reshape(shape))
    return summed.reshape(rows, columns)


def banded(window_high, window_low, band_high, band_low):
    return (
        bf(window_high, band_high, NT)
        + bf(window_low, band_high, NT)
        + bf(window_high, band_low, NT)
    )


def squares(high, low):
    mixed = bf(high, low, NT)
    return bf(high, high, NT) + mixed + mixed.T


def columns_of(block, count=1):
    return pl.ds(pl.multiple_of(block * HB, HB), count * HB)


def first_kernel(
    source, band, offsets, low_s, high_s, low_b, high_b,
    first, upper, lower, gram, high, low, values
):
    width, local = source.shape
    blocks = upper.shape[0]
    for piece, at in ((low_s, 0), (source, 3 * HB), (high_s, 3 * HB + local)):
        part = piece[...]
        where = pl.ds(at, part.shape[1])
        top, bottom = halves(part)
        high[:, where] = top
        low[:, where] = bottom
    first[:width, pl.ds(0, 2 * HB)] = low_s[:, pl.ds(HB, 2 * HB)]
    first[:width, pl.ds(2 * HB, local)] = source[...]
    first[:width, pl.ds(2 * HB + local, 2 * HB)] = high_s[:, pl.ds(0, 2 * HB)]
    values[:, pl.ds(0, 2 * HB)] = low_b[...]
    values[:, pl.ds(2 * HB, local)] = band[...]
    values[:, pl.ds(2 * HB + local, 2 * HB)] = high_b[...]
    diagonals = band.shape[0]
    places = lax.broadcasted_iota(jnp.int32, (diagonals, 3 * HB), 1)
    chosen = jnp.where(places == offsets[...] + HB, 1.0, 0.0).astype(jnp.bfloat16)
    chosen = jnp.concatenate([chosen, chosen], axis=0)

    def step(block, _):
        top, bottom = halves(values[:, columns_of(block)].T)
        spread = bf(jnp.concatenate([top, bottom], axis=1), chosen)
        sheared = pltpu.roll(spread, 0, 1, stride=1, stride_axis=0)
        band_high, band_low = halves(sheared)
        upper[block] = band_high
        lower[block] = band_low
        window = columns_of(block, 3)
        first[width:, columns_of(block)] = banded(
            high[:, window], low[:, window], band_high, band_low
        )
        return 0

    lax.fori_loop(0, blocks, step, 0, unroll=4)
    inner = first[:, pl.ds(2 * HB, local)]
    gram[...] = squares(*halves(inner))


def make_first(source, band, offsets, edges):
    width, local = source.shape
    diagonals = band.shape[0]
    deep = local + 4 * HB
    blocks = deep // HB
    return pl.pallas_call(
        first_kernel,
        out_shape=[
            jax.ShapeDtypeStruct((2 * width, deep), jnp.float32),
            jax.ShapeDtypeStruct((blocks, HB, 3 * HB), jnp.bfloat16),
            jax.ShapeDtypeStruct((blocks, HB, 3 * HB), jnp.bfloat16),
            jax.ShapeDtypeStruct((2 * width, 2 * width), jnp.float32),
        ],
        in_specs=[VMEM] * 7,
        out_specs=[VMEM] * 4,
        scratch_shapes=[
            pltpu.VMEM((width, deep + 2 * HB), jnp.bfloat16),
            pltpu.VMEM((width, deep + 2 * HB), jnp.bfloat16),
            pltpu.VMEM((diagonals, deep), jnp.float32),
        ],
        compiler_params=pltpu.CompilerParams(vmem_limit_bytes=28 << 20),
    )(source, band, offsets.reshape(diagonals, 1), *edges)


def splat(value):
    return jnp.broadcast_to(value, (SUB, LANE))


def eliminate(metric, right):
    tiles = metric.shape[0] // SUB
    part = [slice(SUB * t, SUB * t + SUB) for t in range(tiles)]
    state = [[metric[part[t]], right[part[t]]] for t in range(tiles)]
    rows = lax.broadcasted_iota(jnp.int32, (SUB, LANE), 0)
    solved = []
    steps = range(SUB)
    for t0 in range(tiles):
        at = SUB * t0
        core = {
            (i, k): splat(state[t0][0][i : i + 1, at + k : at + k + 1])
            for i in steps
            for k in range(i, SUB)
        }
        pivots = [[splat(half[i : i + 1]) for half in state[t0]] for i in steps]
        inverse = []
        for i in steps:
            inverse.append(1.0 / core[i, i])
            for k in range(i + 1, SUB):
                ratio = core[i, k] * inverse[i]
                for m in range(k, SUB):
                    core[k, m] = core[k, m] - ratio * core[i, m]
                pivots[k] = [p - ratio * q for p, q in zip(pivots[k], pivots[i])]
        result = jnp.zeros((SUB, LANE), jnp.float32)
        for i in steps:
            result = jnp.where(rows == i, pivots[i][1] * lax.rsqrt(core[i, i]), result)
        solved.append(result)
        for t in range(t0 + 1, tiles):
            scaled = []
            for k in steps:
                column = splat(state[t][0][:, at + k : at + k + 1])
                for i in range(k):
                    column = column - scaled[i] * core[i, k]
                scaled.append(column * inverse[k])
            for half in range(2):
                value = state[t][half]
                for k in steps:
                    value = value - scaled[k] * pivots[k][half]
                state[t][half] = value
    return jnp.concatenate(solved, axis=0)


def compress(grammian, retain):
    spanning = grammian[:retain]
    wide = spanning.shape[1] > retain
    across = lax.broadcasted_iota(jnp.int32, (retain, retain), 1)
    down = lax.broadcasted_iota(jnp.int32, (retain, retain), 0)
    unit = jnp.where(across == down, 1.0, 0.0)
    coeffs = None
    for repeat in range(2):
        if repeat > 0:
            spanning = exact(coeffs, grammian)
        metric = exact(exact(spanning, grammian), spanning, NT)
        metric = 0.5 * (metric + metric.T)
        if wide:
            coeffs = exact(eliminate(metric, unit), spanning)
        else:
            coeffs = eliminate(metric, spanning)
    return coeffs


def second_kernel(
    total, summed, first, upper, lower, factor, squared, corner, gram,
    high, low, once_high, once_low
):
    gram_one = summed[...] * (1.0 / total)
    keep = gram_one.shape[0]
    coeffs = compress(gram_one, keep)
    corner[...] = exact(exact(coeffs, gram_one), coeffs, NT)
    blocks = upper.shape[0]
    local = factor.shape[1]
    width = 4 * HB

    def expand(at, _):
        where = pl.ds(pl.multiple_of(at * width, width), width)
        top, bottom = halves(exact(coeffs, first[:, where]))
        high[:, where] = top
        low[:, where] = bottom
        return 0

    lax.fori_loop(0, first.shape[1] // width, expand, 0)

    def once(block, _):
        window = columns_of(block, 3)
        top, bottom = halves(
            banded(high[:, window], low[:, window], upper[block + 1], lower[block + 1])
        )
        once_high[:, columns_of(block)] = top
        once_low[:, columns_of(block)] = bottom
        return 0

    lax.fori_loop(0, blocks - 2, once, 0, unroll=4)

    def twice(block, _):
        window = columns_of(block, 3)
        squared[:, columns_of(block)] = banded(
            once_high[:, window], once_low[:, window], upper[block + 2], lower[block + 2]
        )
        return 0

    lax.fori_loop(0, blocks - 4, twice, 0, unroll=4)
    middle = pl.ds(2 * HB, local)
    factor[...] = high[:, middle].astype(jnp.float32) + low[:, middle].astype(jnp.float32)
    top, bottom = halves(squared[...])
    gram[:keep] = banded(high[:, middle], low[:, middle], top, bottom)
    gram[keep:] = squares(top, bottom)


def make_second(summed, first, upper, lower, total):
    keep, deep = first.shape
    local = deep - 4 * HB
    shape = jax.ShapeDtypeStruct
    return pl.pallas_call(
        functools.partial(second_kernel, total),
        out_shape=[
            shape((keep, local), jnp.float32),
            shape((keep, local), jnp.float32),
            shape((keep, keep), jnp.float32),
            shape((2 * keep, keep), jnp.float32),
        ],
        in_specs=[VMEM] * 4,
        out_specs=[VMEM] * 4,
        scratch_shapes=[
            pltpu.VMEM((keep, deep), jnp.bfloat16),
            pltpu.VMEM((keep, deep), jnp.bfloat16),
            pltpu.VMEM((keep, deep - 2 * HB), jnp.bfloat16),
            pltpu.VMEM((keep, deep - 2 * HB), jnp.bfloat16),
        ],
        compiler_params=pltpu.CompilerParams(vmem_limit_bytes=28 << 20),
    )(summed, first, upper, lower)


def last_kernel(total, summed, corner, factor, squared, out):
    keep = corner.shape[0]
    cross = summed[:keep] * (1.0 / total)
    own = summed[keep:] * (1.0 / total)
    top = jnp.concatenate([corner[...], cross], axis=1)
    bottom = jnp.concatenate([cross.T, own], axis=1)
    coeffs = compress(jnp.concatenate([top, bottom], axis=0), K2)
    width = 4 * HB

    def step(at, _):
        where = pl.ds(pl.multiple_of(at * width, width), width)
        stacked = jnp.concatenate([factor[:, where], squared[:, where]], axis=0)
        out[:, where] = exact(coeffs, stacked)
        return 0

    lax.fori_loop(0, out.shape[1] // width, step, 0)


def make_last(summed, corner, factor, squared, total):
    return pl.pallas_call(
        functools.partial(last_kernel, total),
        out_shape=jax.ShapeDtypeStruct((K2, factor.shape[1]), jnp.float32),
        in_specs=[VMEM] * 4,
        out_specs=VMEM,
        compiler_params=pltpu.CompilerParams(vmem_limit_bytes=28 << 20),
    )(summed, corner, factor, squared)


def body(source, band_values, offsets):
    total = float(source.shape[1] * lax.axis_size("rows"))
    edges = halos(source, band_values)
    first, upper, lower, gram = make_first(source, band_values, offsets, edges)
    summed = all_total(gram, 1)
    factor, squared, corner, gram = make_second(summed, first, upper, lower, total)
    summed = all_total(gram, 2)
    return make_last(summed, corner, factor, squared, total)


def solution(mesh):
    placed = (P(None, "rows"), P(None, "rows"), P())
    return jax.shard_map(
        body, mesh=mesh, in_specs=placed, out_specs=P(None, "rows"), check_vma=False
    )
```
